32 devices in a mesh: tm: 16 (over z, y, x), state: 2 (over core).
Axes of the slice: x: 2, y: 2, z: 4, core: 2. Of those that a mesh axis runs over, the one named last changes fastest.
Arguments:
- symbols: int32 [8], P('state'), may hold values from 0 to 255
- emission: float32 [8192, 256], P('tm'), may hold values from 0.2 to 5
- decay: float32 [2, 8192], P('state', 'tm'), may hold values from 0.05 to 1
- left_factor: float32 [2, 64, 8192], P('state', None, 'tm'), may hold values from 0.1 to 3
- right_factor: float32 [2, 64, 8192], P('state', None, 'tm'), may hold values from 0.001 to 0.03
- initial: float32 [8192], P('tm'), may hold values from 0.1 to 10
Outputs:
- filtered: float32 [8, 8192], P('state', 'tm')
- log_scale: float32 [8], P('state')
The draws below stay inside these ranges and needn't reach their ends.
All inputs are finite; a program needn't handle non-finite values.
Results may differ from the reference program's by a relative error of at most 0.00011.
Values sent between devices are 32-bit elements; how exact they have to be, the bound alone decides.
No kernel may reach another device: no remote copies, remote signals or barrier semaphores. Data moves between devices by JAX's collectives and lax.ppermute only.
A program may use at most 64 MiB of HBM per device.

```python
import math
import jax
import jax.numpy as jnp
from jax import lax

S = 8192
R = 64
NSYM = 256
F_DEV = 4
SPANS = 2
FRAMES = 8
N_STATE = 2


def plant(entries, own_key, least, top_value):
    dims = entries.shape
    index_at = [jax.random.randint(jax.random.fold_in(own_key, axis), (), 0, dims[axis]) for axis in range(len(dims))]
    entries = entries.at[tuple(index_at)].set(least)
    longest = dims.index(max(dims))
    index_at[longest] = (index_at[longest] + 1) % dims[longest]
    return entries.at[tuple(index_at)].set(top_value)


def level_of(rng, shape, pieces, least, largest):
    loudness, own = 1.0, jax.random.fold_in(rng, 6)
    for position, parts in pieces:
        steps = jnp.exp(jax.random.uniform(jax.random.fold_in(own, position), (parts,), jnp.float32, least / len(pieces), largest / len(pieces)))
        loudness = loudness * jnp.repeat(steps, shape[position] // parts).reshape([-1 if axis == position else 1 for axis in range(len(shape))])
    return loudness


def setup_inputs(seed: int = 0) -> dict:
    keys = jax.random.split(jax.random.key(seed), 7)
    symbols = plant(jax.random.randint(keys[0], (FRAMES,), 0, NSYM), jax.random.fold_in(keys[0], 1), 0, NSYM - 1).astype(jnp.int32)
    emission = jnp.clip(jnp.exp(math.log(5.0) - 3.218876 * jax.random.uniform(keys[1], (S, NSYM), jnp.float32) ** level_of(keys[1], (S, NSYM), ((0, 16),), -0.2, 0.2)), 0.2, 5.0)
    decay = jnp.clip(jnp.exp(math.log(1.0) - 2.9957323 * jax.random.uniform(keys[2], (SPANS, S), jnp.float32) ** level_of(keys[2], (SPANS, S), ((0, 2), (1, 16)), -0.2, 0.2)), 0.05, 1.0)
    left_factor = jnp.clip(jnp.exp(math.log(3.0) - 3.4011974 * jax.random.uniform(keys[3], (SPANS, R, S), jnp.float32) ** level_of(keys[3], (SPANS, R, S), ((0, 2), (2, 16)), -0.2, 0.2)), 0.1, 3.0)
    right_factor = jnp.clip(jnp.exp(math.log(0.03) - 3.4011973 * jax.random.uniform(keys[4], (SPANS, R, S), jnp.float32) ** level_of(keys[4], (SPANS, R, S), ((0, 2), (2, 16)), -0.2, 0.2)), 0.001, 0.03)
    initial = jnp.clip(jnp.exp(math.log(10.0) - 4.6051702 * jax.random.uniform(keys[5], (S,), jnp.float32) ** level_of(keys[5], (S,), ((0, 16),), -0.2, 0.2)), 0.1, 10.0)
    return {"symbols": symbols, "emission": emission, "decay": decay, "left_factor": left_factor, "right_factor": right_factor, "initial": initial}


PRECISE = lax.Precision.HIGHEST


def reference(symbols, emission, decay, left_factor, right_factor, initial):
    belief_init = initial / jnp.mean(initial)

    def block(belief, inputs):
        symbol_row, decay_row, left_rows, right_rows = inputs

        def frame(belief_now, symbol):
            emitted = lax.dynamic_index_in_dim(emission, symbol, 1, keepdims=False)
            mixture = jnp.dot(left_rows, belief_now, precision=PRECISE) / S
            unscaled = emitted * (decay_row * belief_now + jnp.dot(mixture, right_rows, precision=PRECISE))
            normal = jnp.sum(unscaled) / S
            belief_next = unscaled / normal
            return belief_next, (belief_next, jnp.log(normal))

        return lax.scan(frame, belief, symbol_row)

    closing, (beliefs, log_levels) = lax.scan(block, belief_init, (symbols.reshape(N_STATE, F_DEV), decay, left_factor, right_factor))
    return beliefs.reshape(N_STATE * F_DEV, S), log_levels.reshape(N_STATE * F_DEV)
```

```python
import jax
import jax.numpy as jnp
from jax import lax
from jax.experimental import pallas as pl
from jax.experimental.pallas import tpu as pltpu
from jax.sharding import PartitionSpec as P

PRECISE = lax.Precision.HIGHEST
LANES = (((1,), (1,)), ((), ()))
VMEM = pl.BlockSpec(memory_space=pltpu.VMEM)
SMEM = pl.BlockSpec(memory_space=pltpu.SMEM)


def up(count, step):
    return -(-count // step) * step


def dot_lanes(rows, weights):
    return lax.dot_general(
        rows, weights, LANES, precision=PRECISE, preferred_element_type=jnp.float32
    )


def halves(value):
    top = value.astype(jnp.bfloat16)
    return top, (value - top.astype(jnp.float32)).astype(jnp.bfloat16)


def dot_split(rows, weights):
    (row_top, row_low), (top, low) = halves(rows), halves(weights)

    def part(left, right):
        return lax.dot_general(left, right, LANES, preferred_element_type=jnp.float32)

    return part(row_top, top) + (part(row_top, low) + part(row_low, top))


class Plan:
    def __init__(self, frames, rank, members):
        self.frames, self.rank = frames, rank
        self.share = frames // 2
        self.own = [(s, t) for t in range(1, frames) for s in range(t)]
        self.cross = [(s, j) for j in range(self.share) for s in range(frames)]
        self.pairs = len(self.own) + len(self.cross)
        self.tiles = (self.pairs + 1) // 2
        self.levels = [(s, t) for t in range(1, frames + 1) for s in range(t)]
        at = self.tiles * rank
        self.entry_at, at = at, at + up(frames, 8)
        self.own_at, at = at, at + up(len(self.levels), 8)
        self.cross_at, at = at, at + up(len(self.cross), 8)
        self.sum_at, at = at, at + up(frames + 1, 8)
        self.used = at
        self.rows = up(at, 8 * members)
        self.chunk = self.rows // members


def chain(emitted, growth, frames):
    weights = {}
    for s in range(frames):
        weights[s, s + 1] = emitted[s]
        for t in range(s + 2, frames + 1):
            weights[s, t] = weights[s, t - 1] * growth[t - 1]
    reach = [jnp.ones_like(emitted[0])]
    for t in range(frames):
        reach.append(reach[-1] * growth[t])
    return weights, reach


def stack_rows(rows):
    filler = up(len(rows), 8) - len(rows)
    return jnp.concatenate(list(rows) + [jnp.zeros_like(rows[0])] * filler, axis=0)


def both_blocks(first, own, other, rank, frames):
    own_e = [own[rank + f : rank + f + 1] for f in range(frames)]
    other_e = [other[rank + f : rank + f + 1] for f in range(frames)]
    own_d = own[rank + frames : rank + frames + 1]
    other_d = other[rank + frames : rank + frames + 1]
    blocks = []
    for lead in (True, False):
        pick = first if lead else jnp.logical_not(first)
        e = [jnp.where(pick, a, b) for a, b in zip(own_e, other_e)]
        d = jnp.where(pick, own_d, other_d)
        blocks.append((e, d))
    return own_e, own_d, blocks


def offer_kernel(place, symbols, emission, decay, left, right, out):
    frames = symbols.shape[0]
    rank, cells = left.shape
    pad = up(frames, 8)
    at = lax.broadcasted_iota(jnp.int32, (pad, emission.shape[1]), 0)
    lane = lax.broadcasted_iota(jnp.int32, (pad, emission.shape[1]), 1)
    wanted = jnp.full(at.shape, -1, jnp.int32)
    for f in range(frames):
        wanted = jnp.where(at == f, symbols[f], wanted)
    onehot = (lane == wanted).astype(jnp.float32)
    emitted = dot_lanes(onehot, emission[...])
    out[:rank] = jnp.where(place[0] == 0, right[...], left[...])
    rest = [emitted[:frames], decay[...]]
    spare = out.shape[0] - rank - frames - 1
    if spare:
        rest.append(jnp.zeros((spare, cells), jnp.float32))
    out[rank:] = jnp.concatenate(rest, axis=0)


def partial_kernel(plan, place, own_ref, other_ref, left, right, entry, out):
    frames, rank = plan.frames, plan.rank
    first = place[0] == 0
    own_e, own_d, ((e0, d0), (e1, d1)) = both_blocks(
        first, own_ref[rank:], other_ref[rank:], 0, frames
    )
    left_own, right_own = left[...], right[...]
    left_late = jnp.where(first, other_ref[:rank], left_own)
    right_early = jnp.where(first, right_own, other_ref[:rank])
    start = entry[...]
    w_own, _ = chain(own_e, [e * own_d for e in own_e], frames)
    w0, reach0 = chain(e0, [e * d0 for e in e0], frames)
    _, reach1 = chain(e1, [e * d1 for e in e1], frames)
    share = plan.share
    shift = [jnp.where(first, reach1[j], reach1[j + share]) for j in range(share + 1)]
    arrive = [
        start * jnp.where(first, reach0[t], reach0[frames] * reach1[t]) for t in range(frames + 1)
    ]
    own_rows = [right_own * w_own[pair] for pair in plan.own] + [stack_rows(arrive[:frames])]
    cross_w = [w0[s, frames] * shift[j] for s, j in plan.cross]
    cross_rows = [right_early * w for w in cross_w]
    mapped_own = dot_split(jnp.concatenate(own_rows, axis=0), left_own)
    mapped_cross = dot_split(jnp.concatenate(cross_rows, axis=0), left_late)
    many = len(plan.own)
    blocks = [mapped_own[k * rank : (k + 1) * rank] for k in range(many)]
    blocks += [mapped_cross[k * rank : (k + 1) * rank] for k in range(len(plan.cross))]
    if len(blocks) % 2:
        blocks.append(jnp.zeros_like(blocks[0]))
    for k in range(plan.tiles):
        out[k * rank : (k + 1) * rank] = jnp.concatenate(
            [blocks[k], blocks[plan.tiles + k]], axis=1
        )

    def put(at, value):
        out[at : at + value.shape[0]] = jnp.concatenate([value, jnp.zeros_like(value)], axis=1)

    put(plan.entry_at, mapped_own[many * rank :])
    put(plan.own_at, dot_lanes(stack_rows([w_own[pair] for pair in plan.levels]), right_own))
    later = [w0[s, frames] * shift[j + 1] for s, j in plan.cross]
    put(plan.cross_at, dot_lanes(stack_rows(later), right_early))
    totals = jnp.sum(stack_rows(arrive[1:] + [start]), axis=1, keepdims=True)
    out[plan.sum_at : plan.used] = jnp.broadcast_to(totals, (totals.shape[0], out.shape[1]))
    if plan.rows > plan.used:
        out[plan.used :] = jnp.zeros((plan.rows - plan.used, out.shape[1]), jnp.float32)


def solve_kernel(plan, states, place, total, own_ref, other_ref, right, entry, out, logs):
    frames, rank, share, chunk = plan.frames, plan.rank, plan.share, plan.chunk
    first = place[0] == 0
    width = total.shape[3]
    count = 2 * frames

    def rows(core, at, size):
        if at % chunk == 0 and size % chunk == 0:
            return total[at // chunk : (at + size) // chunk, core].reshape(size, width)
        return jnp.concatenate(
            [total[r // chunk, core, r % chunk : r % chunk + 8] for r in range(at, at + size, 8)],
            axis=0,
        )

    lane = lax.broadcasted_iota(jnp.int32, (1, width), 1)
    low = lane < rank
    row_of = lax.broadcasted_iota(jnp.int32, (rank, width), 0)
    lane_of = lax.broadcasted_iota(jnp.int32, (rank, width), 1)
    diagonal = (lane_of == row_of) | (lane_of == row_of + rank)

    feeds = {s: [] for s in range(count)}
    for core in range(2):
        spans = [(core * frames + s, core * frames + t) for s, t in plan.own]
        spans += [(s, frames + core * share + j) for s, j in plan.cross]
        for k, (s, t) in enumerate(spans):
            feeds[s].append((core, k % plan.tiles, k < plan.tiles, t))

    entries = [rows(core, plan.entry_at, up(frames, 8)) for core in range(2)]
    acc = [entries[t // frames][t % frames : t % frames + 1] for t in range(count)]
    cols, lines = [], []
    for s in range(count):
        line = acc[s] * (1.0 / states)
        cols.append(jnp.sum(jnp.where(diagonal, line, 0.0), axis=1, keepdims=True))
        lines.append(jnp.where(low, line + pltpu.roll(line, rank, 1), 0.0))
        for core, tile, lower, t in feeds[s]:
            gain = jnp.sum(rows(core, tile * rank, rank) * cols[s], axis=0, keepdims=True)
            acc[t] = acc[t] + jnp.where(low if lower else ~low, gain, 0.0)

    level_rows = [jnp.zeros((1, width), jnp.float32) for _ in range(count)]
    for core in range(2):
        weights = rows(core, plan.own_at, up(len(plan.levels), 8))
        for k, (s, t) in enumerate(plan.levels):
            at = core * frames + t - 1
            level_rows[at] = level_rows[at] + weights[k : k + 1] * lines[core * frames + s]
        weights = rows(core, plan.cross_at, up(len(plan.cross), 8))
        for k, (s, j) in enumerate(plan.cross):
            at = frames + core * share + j
            level_rows[at] = level_rows[at] + weights[k : k + 1] * lines[s]
    totals = [rows(core, plan.sum_at, up(frames + 1, 8)) for core in range(2)]
    base = jnp.concatenate(
        [totals[0][frames : frames + 1], totals[0][:frames], totals[1][:frames]], axis=0
    )
    mixed = jnp.sum(jnp.concatenate(level_rows, axis=0), axis=1, keepdims=True)
    levels = [base[:1]] + [base[t + 1 : t + 2] + mixed[t : t + 1] for t in range(count)]

    own_e, own_d, ((e0, d0), (e1, d1)) = both_blocks(
        first, own_ref[rank:], other_ref[rank:], 0, frames
    )
    right_own = right[...]
    right_early = jnp.where(first, right_own, other_ref[:rank])
    belief = entry[...]
    found = []
    for t in range(count):
        e, d = (e0[t], d0) if t < frames else (e1[t - frames], d1)
        factor = right_early if t < frames else right_own
        belief = e * (d * belief + jnp.sum(factor * cols[t], axis=0, keepdims=True))
        found.append(belief)
    for f in range(frames):
        scale = jnp.where(first, levels[f + 1], levels[frames + f + 1])[:, :1]
        before = jnp.where(first, levels[f], levels[frames + f])
        after = jnp.where(first, levels[f + 1], levels[frames + f + 1])
        out[f : f + 1] = jnp.where(first, found[f], found[frames + f]) * (states / scale)
        logs[f : f + 1] = jnp.log(after / before)


def solution(mesh):
    members = mesh.shape["tm"]
    cores = mesh.shape["state"]
    assert cores == 2

    def per_device(symbols, emission, decay, left_factor, right_factor, initial):
        left, right = left_factor[0], right_factor[0]
        frames = symbols.shape[0]
        rank, cells = left.shape
        states = members * cells
        plan = Plan(frames, rank, members)
        width = 2 * rank
        place = lax.axis_index("state").astype(jnp.int32).reshape(1)
        entry = initial.reshape(1, cells)
        offered = pl.pallas_call(
            offer_kernel,
            out_shape=jax.ShapeDtypeStruct((up(rank + frames + 1, 8), cells), jnp.float32),
            in_specs=[SMEM, SMEM, VMEM, VMEM, VMEM, VMEM],
            out_specs=VMEM,
            name="offer",
        )(place, symbols, emission, decay, left, right)
        other = lax.ppermute(offered, "state", [(0, 1), (1, 0)])
        partial = pl.pallas_call(
            lambda *refs: partial_kernel(plan, *refs),
            out_shape=jax.ShapeDtypeStruct((plan.rows, width), jnp.float32),
            in_specs=[SMEM] + [VMEM] * 5,
            out_specs=VMEM,
            name="partial",
        )(place, offered, other, left, right, entry)
        parts = lax.all_to_all(partial, "tm", 0, 0, tiled=True)
        mine = jnp.sum(parts.reshape(members, plan.chunk, width), axis=0)
        copies = jnp.broadcast_to(mine[None], (members * cores, plan.chunk, width))
        total = lax.all_to_all(copies, ("tm", "state"), 0, 0, tiled=True)
        beliefs, logs = pl.pallas_call(
            lambda *refs: solve_kernel(plan, states, *refs),
            out_shape=(
                jax.ShapeDtypeStruct((frames, cells), jnp.float32),
                jax.ShapeDtypeStruct((frames, width), jnp.float32),
            ),
            in_specs=[SMEM] + [VMEM] * 5,
            out_specs=(VMEM, VMEM),
            name="solve",
        )(place, total.reshape(members, cores, plan.chunk, width), offered, other, right, entry)
        return beliefs, logs[:, 0]

    return jax.shard_map(
        per_device,
        mesh=mesh,
        in_specs=(
            P("state"),
            P("tm", None),
            P("state", "tm"),
            P("state", None, "tm"),
            P("state", None, "tm"),
            P("tm"),
        ),
        out_specs=(P("state", "tm"), P("state")),
        check_vma=False,
    )
```

```python
import jax
import jax.numpy as jnp
from jax import lax
from jax.experimental import pallas as pl
from jax.experimental.pallas import tpu as pltpu
from jax.sharding import PartitionSpec as P

PRECISE = lax.Precision.HIGHEST
LANES = (((1,), (1,)), ((), ()))
VMEM = pl.BlockSpec(memory_space=pltpu.VMEM)
SMEM = pl.BlockSpec(memory_space=pltpu.SMEM)


def up(count, step):
    return -(-count // step) * step


def dot_lanes(rows, weights):
    return lax.dot_general(
        rows, weights, LANES, precision=PRECISE, preferred_element_type=jnp.float32
    )


def halves(value):
    top = value.astype(jnp.bfloat16)
    return top, (value - top.astype(jnp.float32)).astype(jnp.bfloat16)


def dot_split(rows, weights):
    (row_top, row_low), (top, low) = halves(rows), halves(weights)

    def part(left, right):
        return lax.dot_general(left, right, LANES, preferred_element_type=jnp.float32)

    return part(row_top, top) + (part(row_top, low) + part(row_low, top))


class Plan:
    def __init__(self, frames, rank, members):
        self.frames, self.rank = frames, rank
        self.share = frames // 2
        self.own = [(s, t) for t in range(1, frames) for s in range(t)]
        self.cross = [(s, j) for j in range(self.share) for s in range(frames)]
        self.pairs = len(self.own) + len(self.cross)
        self.tiles = (self.pairs + 1) // 2
        self.levels = [(s, t) for t in range(1, frames + 1) for s in range(t)]
        at = self.tiles * rank
        self.entry_at, at = at, at + up(frames, 8)
        self.own_at, at = at, at + up(len(self.levels), 8)
        self.cross_at, at = at, at + up(len(self.cross), 8)
        self.sum_at, at = at, at + up(frames + 1, 8)
        self.used = at
        self.rows = up(at, 8 * members)
        self.chunk = self.rows // members


def chain(emitted, growth, frames):
    weights = {}
    for s in range(frames):
        weights[s, s + 1] = emitted[s]
        for t in range(s + 2, frames + 1):
            weights[s, t] = weights[s, t - 1] * growth[t - 1]
    reach = [jnp.ones_like(emitted[0])]
    for t in range(frames):
        reach.append(reach[-1] * growth[t])
    return weights, reach


def stack_rows(rows):
    filler = up(len(rows), 8) - len(rows)
    return jnp.concatenate(list(rows) + [jnp.zeros_like(rows[0])] * filler, axis=0)


def offer_kernel(place, symbols, decay, left, right, out):
    frames = symbols.shape[0]
    rank, cells = left.shape
    spare = out.shape[0] - rank - frames - 1
    out[:rank] = jnp.where(place[0] == 0, right[...], left[...])
    rest = [decay[...]]
    rest += [jnp.full((1, cells), symbols[f].astype(jnp.float32)) for f in range(frames)]
    rest += [jnp.zeros((1, cells), jnp.float32)] * spare
    out[rank:] = jnp.concatenate(rest, axis=0)


def in_order(first, own, other):
    return jnp.where(first, own, other), jnp.where(first, other, own)


def partial_kernel(plan, place, own_ref, other_ref, emission, left, right, entry, out, seen):
    frames, rank = plan.frames, plan.rank
    first = place[0] == 0
    own_d = own_ref[rank : rank + 1]
    d0, d1 = in_order(first, own_d, other_ref[rank : rank + 1])
    early, late = in_order(first, own_ref[rank:, :1], other_ref[rank:, :1])
    shape = (seen.shape[0], emission.shape[1])
    at = lax.broadcasted_iota(jnp.int32, shape, 0)
    wanted = jnp.full(shape, -1.0, jnp.float32)
    for f in range(frames):
        wanted = jnp.where(at == f, early[1 + f : 2 + f], wanted)
        wanted = jnp.where(at == frames + f, late[1 + f : 2 + f], wanted)
    symbol = lax.broadcasted_iota(jnp.int32, shape, 1).astype(jnp.float32)
    emitted = dot_lanes((symbol == wanted).astype(jnp.float32), emission[...])
    seen[...] = emitted
    e0 = [emitted[f : f + 1] for f in range(frames)]
    e1 = [emitted[frames + f : frames + f + 1] for f in range(frames)]
    own_e = [jnp.where(first, a, b) for a, b in zip(e0, e1)]
    left_own, right_own = left[...], right[...]
    left_late = jnp.where(first, other_ref[:rank], left_own)
    right_early = jnp.where(first, right_own, other_ref[:rank])
    start = entry[...]
    w_own, _ = chain(own_e, [e * own_d for e in own_e], frames)
    w0, reach0 = chain(e0, [e * d0 for e in e0], frames)
    _, reach1 = chain(e1, [e * d1 for e in e1], frames)
    share = plan.share
    shift = [jnp.where(first, reach1[j], reach1[j + share]) for j in range(share + 1)]
    arrive = [
        start * jnp.where(first, reach0[t], reach0[frames] * reach1[t]) for t in range(frames + 1)
    ]
    own_rows = [right_own * w_own[pair] for pair in plan.own] + [stack_rows(arrive[:frames])]
    cross_w = [w0[s, frames] * shift[j] for s, j in plan.cross]
    cross_rows = [right_early * w for w in cross_w]
    mapped_own = dot_split(jnp.concatenate(own_rows, axis=0), left_own)
    mapped_cross = dot_split(jnp.concatenate(cross_rows, axis=0), left_late)
    many = len(plan.own)
    blocks = [mapped_own[k * rank : (k + 1) * rank] for k in range(many)]
    blocks += [mapped_cross[k * rank : (k + 1) * rank] for k in range(len(plan.cross))]
    if len(blocks) % 2:
        blocks.append(jnp.zeros_like(blocks[0]))
    for k in range(plan.tiles):
        out[k * rank : (k + 1) * rank] = jnp.concatenate(
            [blocks[k], blocks[plan.tiles + k]], axis=1
        )

    def put(at, value):
        out[at : at + value.shape[0]] = jnp.concatenate([value, jnp.zeros_like(value)], axis=1)

    put(plan.entry_at, mapped_own[many * rank :])
    put(plan.own_at, dot_lanes(stack_rows([w_own[pair] for pair in plan.levels]), right_own))
    later = [w0[s, frames] * shift[j + 1] for s, j in plan.cross]
    put(plan.cross_at, dot_lanes(stack_rows(later), right_early))
    totals = jnp.sum(stack_rows(arrive[1:] + [start]), axis=1, keepdims=True)
    out[plan.sum_at : plan.used] = jnp.broadcast_to(totals, (totals.shape[0], out.shape[1]))
    if plan.rows > plan.used:
        out[plan.used :] = jnp.zeros((plan.rows - plan.used, out.shape[1]), jnp.float32)


def solve_kernel(
    plan, states, place, mine, theirs, own_ref, other_ref, seen, right, entry, out, logs
):
    frames, rank, share = plan.frames, plan.rank, plan.share
    first = place[0] == 0
    width = mine.shape[1]
    count = 2 * frames

    def rows(core, at, size):
        return in_order(first, mine[at : at + size], theirs[at : at + size])[core]

    lane = lax.broadcasted_iota(jnp.int32, (1, width), 1)
    low = lane < rank
    row_of = lax.broadcasted_iota(jnp.int32, (rank, width), 0)
    lane_of = lax.broadcasted_iota(jnp.int32, (rank, width), 1)
    diagonal = (lane_of == row_of) | (lane_of == row_of + rank)

    feeds = {s: [] for s in range(count)}
    for core in range(2):
        spans = [(core * frames + s, core * frames + t) for s, t in plan.own]
        spans += [(s, frames + core * share + j) for s, j in plan.cross]
        for k, (s, t) in enumerate(spans):
            feeds[s].append((core, k % plan.tiles, k < plan.tiles, t))

    entries = [rows(core, plan.entry_at, up(frames, 8)) for core in range(2)]
    acc = [entries[t // frames][t % frames : t % frames + 1] for t in range(count)]
    cols, lines = [], []
    for s in range(count):
        line = acc[s] * (1.0 / states)
        cols.append(jnp.sum(jnp.where(diagonal, line, 0.0), axis=1, keepdims=True))
        lines.append(jnp.where(low, line + pltpu.roll(line, rank, 1), 0.0))
        for core, tile, lower, t in feeds[s]:
            gain = jnp.sum(rows(core, tile * rank, rank) * cols[s], axis=0, keepdims=True)
            acc[t] = acc[t] + jnp.where(low if lower else ~low, gain, 0.0)

    level_rows = [jnp.zeros((1, width), jnp.float32) for _ in range(count)]
    for core in range(2):
        weights = rows(core, plan.own_at, up(len(plan.levels), 8))
        for k, (s, t) in enumerate(plan.levels):
            at = core * frames + t - 1
            level_rows[at] = level_rows[at] + weights[k : k + 1] * lines[core * frames + s]
        weights = rows(core, plan.cross_at, up(len(plan.cross), 8))
        for k, (s, j) in enumerate(plan.cross):
            at = frames + core * share + j
            level_rows[at] = level_rows[at] + weights[k : k + 1] * lines[s]
    totals = [rows(core, plan.sum_at, up(frames + 1, 8)) for core in range(2)]
    base = jnp.concatenate(
        [totals[0][frames : frames + 1], totals[0][:frames], totals[1][:frames]], axis=0
    )
    mixed = jnp.sum(jnp.concatenate(level_rows, axis=0), axis=1, keepdims=True)
    levels = [base[:1]] + [base[t + 1 : t + 2] + mixed[t : t + 1] for t in range(count)]

    d0, d1 = in_order(first, own_ref[rank : rank + 1], other_ref[rank : rank + 1])
    right_own = right[...]
    right_early = jnp.where(first, right_own, other_ref[:rank])
    belief = entry[...]
    found = []
    for t in range(count):
        e, d = seen[t : t + 1], d0 if t < frames else d1
        factor = right_early if t < frames else right_own
        belief = e * (d * belief + jnp.sum(factor * cols[t], axis=0, keepdims=True))
        found.append(belief)
    for f in range(frames):
        scale = jnp.where(first, levels[f + 1], levels[frames + f + 1])[:, :1]
        before = jnp.where(first, levels[f], levels[frames + f])
        after = jnp.where(first, levels[f + 1], levels[frames + f + 1])
        out[f : f + 1] = jnp.where(first, found[f], found[frames + f]) * (states / scale)
        logs[f] = jnp.log(after / before)[0, 0]


def solution(mesh):
    members = mesh.shape["tm"]
    cores = mesh.shape["state"]
    assert cores == 2

    def per_device(symbols, emission, decay, left_factor, right_factor, initial):
        left, right = left_factor[0], right_factor[0]
        frames = symbols.shape[0]
        rank, cells = left.shape
        states = members * cells
        plan = Plan(frames, rank, members)
        width = 2 * rank
        place = lax.axis_index("state").astype(jnp.int32).reshape(1)
        entry = initial.reshape(1, cells)
        offered = pl.pallas_call(
            offer_kernel,
            out_shape=jax.ShapeDtypeStruct((up(rank + frames + 1, 8), cells), jnp.float32),
            in_specs=[SMEM, SMEM, VMEM, VMEM, VMEM],
            out_specs=VMEM,
            name="offer",
        )(place, symbols, decay, left, right)
        other = lax.ppermute(offered, "state", [(0, 1), (1, 0)])
        partial, seen = pl.pallas_call(
            lambda *refs: partial_kernel(plan, *refs),
            out_shape=(
                jax.ShapeDtypeStruct((plan.rows, width), jnp.float32),
                jax.ShapeDtypeStruct((up(2 * frames, 8), cells), jnp.float32),
            ),
            in_specs=[SMEM] + [VMEM] * 6,
            out_specs=(VMEM, VMEM),
            name="partial",
        )(place, offered, other, emission, left, right, entry)
        parts = lax.all_to_all(partial, "tm", 0, 0, tiled=True)
        chunk = jnp.sum(parts.reshape(members, plan.chunk, width), axis=0)
        copies = jnp.broadcast_to(chunk[None], (members, plan.chunk, width))
        mine = lax.all_to_all(copies, "tm", 0, 0, tiled=True).reshape(plan.rows, width)
        theirs = lax.ppermute(mine, "state", [(0, 1), (1, 0)])
        return pl.pallas_call(
            lambda *refs: solve_kernel(plan, states, *refs),
            out_shape=(
                jax.ShapeDtypeStruct((frames, cells), jnp.float32),
                jax.ShapeDtypeStruct((frames,), jnp.float32),
            ),
            in_specs=[SMEM] + [VMEM] * 7,
            out_specs=(VMEM, SMEM),
            name="solve",
        )(place, mine, theirs, offered, other, seen, right, entry)

    return jax.shard_map(
        per_device,
        mesh=mesh,
        in_specs=(
            P("state"),
            P("tm", None),
            P("state", "tm"),
            P("state", None, "tm"),
            P("state", None, "tm"),
            P("tm"),
        ),
        out_specs=(P("state", "tm"), P("state")),
        check_vma=False,
    )
```

```python
import jax
import jax.numpy as jnp
from jax import lax
from jax.experimental import pallas as pl
from jax.experimental.pallas import tpu as pltpu
from jax.sharding import PartitionSpec as P

PRECISE = lax.Precision.HIGHEST
LANES = (((1,), (1,)), ((), ()))
VMEM = pl.BlockSpec(memory_space=pltpu.VMEM)
SMEM = pl.BlockSpec(memory_space=pltpu.SMEM)


def near(value):
    return pltpu.with_memory_space_constraint(value, pltpu.VMEM)


def up(count, step):
    return -(-count // step) * step


def dot_lanes(rows, weights):
    return lax.dot_general(
        rows, weights, LANES, precision=PRECISE, preferred_element_type=jnp.float32
    )


def halves(value):
    top = value.astype(jnp.bfloat16)
    return top, (value - top.astype(jnp.float32)).astype(jnp.bfloat16)


def dot_split(rows, weights):
    (row_top, row_low), (top, low) = halves(rows), halves(weights)

    def part(left, right):
        return lax.dot_general(left, right, LANES, preferred_element_type=jnp.float32)

    return part(row_top, top) + (part(row_top, low) + part(row_low, top))


class Plan:
    def __init__(self, frames, rank, members):
        self.frames, self.rank = frames, rank
        self.share = frames // 2
        self.own = [(s, t) for t in range(1, frames) for s in range(t)]
        self.cross = [(s, j) for j in range(self.share) for s in range(frames)]
        self.pairs = len(self.own) + len(self.cross)
        self.tiles = (self.pairs + 1) // 2
        self.levels = [(s, t) for t in range(1, frames + 1) for s in range(t)]
        at = self.tiles * rank
        self.entry_at, at = at, at + up(frames, 8)
        self.own_at, at = at, at + up(len(self.levels), 8)
        self.cross_at, at = at, at + up(len(self.cross), 8)
        self.sum_at, at = at, at + up(frames + 1, 8)
        self.used = at
        self.rows = up(at, 8 * members)
        self.chunk = self.rows // members


def chain(emitted, growth, frames):
    weights = {}
    for s in range(frames):
        weights[s, s + 1] = emitted[s]
        for t in range(s + 2, frames + 1):
            weights[s, t] = weights[s, t - 1] * growth[t - 1]
    reach = [jnp.ones_like(emitted[0])]
    for t in range(frames):
        reach.append(reach[-1] * growth[t])
    return weights, reach


def stack_rows(rows):
    filler = up(len(rows), 8) - len(rows)
    return jnp.concatenate(list(rows) + [jnp.zeros_like(rows[0])] * filler, axis=0)


def offer_kernel(place, symbols, decay, left, right, out):
    frames = symbols.shape[0]
    rank, cells = left.shape
    spare = out.shape[0] - rank - frames - 1
    out[:rank] = jnp.where(place[0] == 0, right[...], left[...])
    rest = [decay[...]]
    rest += [jnp.full((1, cells), symbols[f].astype(jnp.float32)) for f in range(frames)]
    rest += [jnp.zeros((1, cells), jnp.float32)] * spare
    out[rank:] = jnp.concatenate(rest, axis=0)


def in_order(first, own, other):
    return jnp.where(first, own, other), jnp.where(first, other, own)


def partial_kernel(plan, place, own_ref, other_ref, emission, left, right, entry, out, seen):
    frames, rank = plan.frames, plan.rank
    first = place[0] == 0
    own_d = own_ref[rank : rank + 1]
    d0, d1 = in_order(first, own_d, other_ref[rank : rank + 1])
    early, late = in_order(first, own_ref[rank:, :1], other_ref[rank:, :1])
    shape = (seen.shape[0], emission.shape[1])
    at = lax.broadcasted_iota(jnp.int32, shape, 0)
    wanted = jnp.full(shape, -1.0, jnp.float32)
    for f in range(frames):
        wanted = jnp.where(at == f, early[1 + f : 2 + f], wanted)
        wanted = jnp.where(at == frames + f, late[1 + f : 2 + f], wanted)
    symbol = lax.broadcasted_iota(jnp.int32, shape, 1).astype(jnp.float32)
    emitted = dot_lanes((symbol == wanted).astype(jnp.float32), emission[...])
    seen[...] = emitted
    e0 = [emitted[f : f + 1] for f in range(frames)]
    e1 = [emitted[frames + f : frames + f + 1] for f in range(frames)]
    own_e = [jnp.where(first, a, b) for a, b in zip(e0, e1)]
    left_own, right_own = left[...], right[...]
    left_late = jnp.where(first, other_ref[:rank], left_own)
    right_early = jnp.where(first, right_own, other_ref[:rank])
    start = entry[...]
    w_own, _ = chain(own_e, [e * own_d for e in own_e], frames)
    w0, reach0 = chain(e0, [e * d0 for e in e0], frames)
    _, reach1 = chain(e1, [e * d1 for e in e1], frames)
    share = plan.share
    shift = [jnp.where(first, reach1[j], reach1[j + share]) for j in range(share + 1)]
    arrive = [
        start * jnp.where(first, reach0[t], reach0[frames] * reach1[t]) for t in range(frames + 1)
    ]
    own_rows = [right_own * w_own[pair] for pair in plan.own] + [stack_rows(arrive[:frames])]
    cross_w = [w0[s, frames] * shift[j] for s, j in plan.cross]
    cross_rows = [right_early * w for w in cross_w]
    mapped_own = dot_split(jnp.concatenate(own_rows, axis=0), left_own)
    mapped_cross = dot_split(jnp.concatenate(cross_rows, axis=0), left_late)
    many = len(plan.own)
    blocks = [mapped_own[k * rank : (k + 1) * rank] for k in range(many)]
    blocks += [mapped_cross[k * rank : (k + 1) * rank] for k in range(len(plan.cross))]
    if len(blocks) % 2:
        blocks.append(jnp.zeros_like(blocks[0]))
    for k in range(plan.tiles):
        out[k * rank : (k + 1) * rank] = jnp.concatenate(
            [blocks[k], blocks[plan.tiles + k]], axis=1
        )

    def put(at, value):
        out[at : at + value.shape[0]] = jnp.concatenate([value, jnp.zeros_like(value)], axis=1)

    put(plan.entry_at, mapped_own[many * rank :])
    put(plan.own_at, dot_lanes(stack_rows([w_own[pair] for pair in plan.levels]), right_own))
    later = [w0[s, frames] * shift[j + 1] for s, j in plan.cross]
    put(plan.cross_at, dot_lanes(stack_rows(later), right_early))
    totals = jnp.sum(stack_rows(arrive[1:] + [start]), axis=1, keepdims=True)
    out[plan.sum_at : plan.used] = jnp.broadcast_to(totals, (totals.shape[0], out.shape[1]))
    if plan.rows > plan.used:
        out[plan.used :] = jnp.zeros((plan.rows - plan.used, out.shape[1]), jnp.float32)


def solve_kernel(
    plan, states, place, mine, theirs, own_ref, other_ref, seen, right, entry, out, logs
):
    frames, rank, share = plan.frames, plan.rank, plan.share
    first = place[0] == 0
    width = mine.shape[1]
    count = 2 * frames

    def rows(core, at, size):
        return in_order(first, mine[at : at + size], theirs[at : at + size])[core]

    lane = lax.broadcasted_iota(jnp.int32, (1, width), 1)
    low = lane < rank
    row_of = lax.broadcasted_iota(jnp.int32, (rank, width), 0)
    lane_of = lax.broadcasted_iota(jnp.int32, (rank, width), 1)
    diagonal = (lane_of == row_of) | (lane_of == row_of + rank)

    feeds = {s: [] for s in range(count)}
    for core in range(2):
        spans = [(core * frames + s, core * frames + t) for s, t in plan.own]
        spans += [(s, frames + core * share + j) for s, j in plan.cross]
        for k, (s, t) in enumerate(spans):
            feeds[s].append((core, k % plan.tiles, k < plan.tiles, t))

    entries = [rows(core, plan.entry_at, up(frames, 8)) for core in range(2)]
    acc = [entries[t // frames][t % frames : t % frames + 1] for t in range(count)]
    cols, lines = [], []
    for s in range(count):
        line = acc[s] * (1.0 / states)
        cols.append(jnp.sum(jnp.where(diagonal, line, 0.0), axis=1, keepdims=True))
        lines.append(jnp.where(low, line + pltpu.roll(line, rank, 1), 0.0))
        for core, tile, lower, t in feeds[s]:
            gain = jnp.sum(rows(core, tile * rank, rank) * cols[s], axis=0, keepdims=True)
            acc[t] = acc[t] + jnp.where(low if lower else ~low, gain, 0.0)

    level_rows = [jnp.zeros((1, width), jnp.float32) for _ in range(count)]
    for core in range(2):
        weights = rows(core, plan.own_at, up(len(plan.levels), 8))
        for k, (s, t) in enumerate(plan.levels):
            at = core * frames + t - 1
            level_rows[at] = level_rows[at] + weights[k : k + 1] * lines[core * frames + s]
        weights = rows(core, plan.cross_at, up(len(plan.cross), 8))
        for k, (s, j) in enumerate(plan.cross):
            at = frames + core * share + j
            level_rows[at] = level_rows[at] + weights[k : k + 1] * lines[s]
    totals = [rows(core, plan.sum_at, up(frames + 1, 8)) for core in range(2)]
    base = jnp.concatenate(
        [totals[0][frames : frames + 1], totals[0][:frames], totals[1][:frames]], axis=0
    )
    mixed = jnp.sum(jnp.concatenate(level_rows, axis=0), axis=1, keepdims=True)
    levels = [base[:1]] + [base[t + 1 : t + 2] + mixed[t : t + 1] for t in range(count)]

    d0, d1 = in_order(first, own_ref[rank : rank + 1], other_ref[rank : rank + 1])
    right_own = right[...]
    right_early = jnp.where(first, right_own, other_ref[:rank])
    belief = entry[...]
    found = []
    for t in range(count):
        e, d = seen[t : t + 1], d0 if t < frames else d1
        factor = right_early if t < frames else right_own
        belief = e * (d * belief + jnp.sum(factor * cols[t], axis=0, keepdims=True))
        found.append(belief)
    for f in range(frames):
        scale = jnp.where(first, levels[f + 1], levels[frames + f + 1])[:, :1]
        before = jnp.where(first, levels[f], levels[frames + f])
        after = jnp.where(first, levels[f + 1], levels[frames + f + 1])
        out[f : f + 1] = jnp.where(first, found[f], found[frames + f]) * (states / scale)
        logs[f] = jnp.log(after / before)[0, 0]


def solution(mesh):
    members = mesh.shape["tm"]
    cores = mesh.shape["state"]
    assert cores == 2

    def per_device(symbols, emission, decay, left_factor, right_factor, initial):
        left, right = near(left_factor[0]), near(right_factor[0])
        frames = symbols.shape[0]
        rank, cells = left.shape
        states = members * cells
        plan = Plan(frames, rank, members)
        width = 2 * rank
        place = lax.axis_index("state").astype(jnp.int32).reshape(1)
        entry = near(initial.reshape(1, cells))
        emission = near(emission)
        offered = pl.pallas_call(
            offer_kernel,
            out_shape=pltpu.VMEM((up(rank + frames + 1, 8), cells), jnp.float32),
            in_specs=[SMEM, SMEM, VMEM, VMEM, VMEM],
            out_specs=VMEM,
            name="offer",
        )(place, symbols, decay, left, right)
        other = lax.ppermute(offered, "state", [(0, 1), (1, 0)])
        partial, seen = pl.pallas_call(
            lambda *refs: partial_kernel(plan, *refs),
            out_shape=(
                pltpu.VMEM((plan.rows, width), jnp.float32),
                pltpu.VMEM((up(2 * frames, 8), cells), jnp.float32),
            ),
            in_specs=[SMEM] + [VMEM] * 6,
            out_specs=(VMEM, VMEM),
            name="partial",
        )(place, near(offered), near(other), emission, left, right, entry)
        parts = lax.all_to_all(partial, "tm", 0, 0, tiled=True)
        chunk = jnp.sum(parts.reshape(members, plan.chunk, width), axis=0)
        copies = jnp.broadcast_to(chunk[None], (members, plan.chunk, width))
        mine = lax.all_to_all(copies, "tm", 0, 0, tiled=True).reshape(plan.rows, width)
        theirs = lax.ppermute(mine, "state", [(0, 1), (1, 0)])
        return pl.pallas_call(
            lambda *refs: solve_kernel(plan, states, *refs),
            out_shape=(
                jax.ShapeDtypeStruct((frames, cells), jnp.float32),
                jax.ShapeDtypeStruct((frames,), jnp.float32),
            ),
            in_specs=[SMEM] + [VMEM] * 7,
            out_specs=(VMEM, SMEM),
            name="solve",
        )(place, near(mine), near(theirs), near(offered), near(other), near(seen), right, entry)

    return jax.shard_map(
        per_device,
        mesh=mesh,
        in_specs=(
            P("state"),
            P("tm", None),
            P("state", "tm"),
            P("state", None, "tm"),
            P("state", None, "tm"),
            P("tm"),
        ),
        out_specs=(P("state", "tm"), P("state")),
        check_vma=False,
    )
```
